128 devices in a mesh: groups: 4 (over x, y), lon: 16 (over z), lat: 2 (over core).
Axes of the slice: x: 2, y: 2, z: 16, core: 2. Of those that a mesh axis runs over, the one named last changes fastest.
The devices are a block of a 8x8x16 slice.
Arguments:
- fields: bfloat16 [48, 2048, 128], P(('groups', 'lat'), 'lon'), parts along dimension 0, may hold values from -6 to 6
- norm_gain: float32 [128], replicated, may hold values from 0.5 to 1.5
- w_qkv: bfloat16 [128, 384], replicated, may hold values from -5.303301 to 5.303301
- w_out: bfloat16 [128, 128], replicated, may hold values from -0.5 to 0.5
Outputs:
- updated: bfloat16 [48, 2048, 128], P(('groups', 'lat'), 'lon'), parts along dimension 0
The draws below stay inside these ranges and needn't reach their ends.
There are 4 independent parts, one for each index of `groups`. The reference program is written for one: setup_inputs(seed, part) draws one part's arguments, and reference() takes and returns one part's arrays. A program takes and returns all parts, laid end to end along the dimension named above; an argument that names none is the same for every part. Nothing has to cross between parts.
All inputs are finite; a program needn't handle non-finite values.
Results may differ from the reference program's by a relative error of at most 0.005.
The reference program's roundings to bfloat16 on the way (of `normed`, `weights` and `attended`) count: a program that leaves them out, or rounds other values in their place, can miss the bound.
Values may be sent and summed in bfloat16 or wider, within the bound.
No kernel may reach another device: no remote copies, remote signals or barrier semaphores. Data moves between devices by JAX's collectives and lax.ppermute only.
A program may use at most 128 MiB of HBM per device.

```python
import math
import jax
import jax.numpy as jnp
from jax import lax

HEADS = 8
HEAD_DIM = 16
C = 128
NLON = 2048
NLAT = 12


def draw_w_qkv(key, part):
    base = jnp.clip(jax.random.normal(key, (C, 3 * C), jnp.float32), -6.0, 6.0) * (2.0 / math.sqrt(C))
    return base.astype(jnp.bfloat16)


def block_scale(stream_key, shape, shards, low, high):
    def one(position, shards_of):
        steps = jax.random.uniform(jax.random.fold_in(jax.random.fold_in(stream_key, 6), position), (shards_of,), jnp.float32, low / len(shards), high / len(shards))
        return jnp.repeat(jnp.exp(steps), shape[position] // shards_of).reshape((-1,) + (1,) * (len(shape) - position - 1))

    loudness = one(*shards[0])
    for cut in shards[1:]:
        loudness = loudness * one(*cut)
    return loudness


def bell_draw(rng, dims, scale, bound, split=(), kind=jnp.bfloat16):
    values = scale * jax.random.normal(rng, dims, jnp.float32)
    if split:
        values = values * block_scale(rng, dims, split, -0.22, 0.18)
    return jnp.clip(values, -bound, bound).astype(kind)


def setup_inputs(seed: int = 0, part: int = 0) -> dict:
    key_list = jax.random.split(jax.random.key(seed), 5)
    part_keys = jax.random.split(jax.random.fold_in(key_list[4], part), 5)
    fields = bell_draw(part_keys[0], (NLAT, NLON, C), 1.0, 6.0, ((0, 2), (1, 16)))
    norm_gain = jnp.clip(1.0 + 0.1 * jax.random.normal(key_list[1], (C,), jnp.float32), 0.5, 1.5)
    w_qkv = draw_w_qkv(jax.random.fold_in(key_list[4], 71), part)
    w_out = bell_draw(key_list[3], (C, C), C ** -0.5, 0.5)
    return {"fields": fields, "norm_gain": norm_gain, "w_qkv": w_qkv, "w_out": w_out}


def reference(fields, norm_gain, w_qkv, w_out):
    width = HEADS * HEAD_DIM
    inputs = fields.astype(jnp.float32)
    center = lax.optimization_barrier(jnp.mean(inputs, axis=-1, keepdims=True))
    spread = lax.optimization_barrier(jnp.mean((inputs - center) ** 2, axis=-1, keepdims=True))
    normed = ((inputs - center) * lax.rsqrt(spread + 1e-05) * norm_gain).astype(jnp.bfloat16)
    projected = jnp.dot(normed.reshape(-1, width), w_qkv, preferred_element_type=jnp.float32)
    projected = projected.reshape(NLAT, NLON, 3 * width)
    queries = (projected[..., :width] * (1.0 / math.sqrt(HEAD_DIM))).astype(jnp.bfloat16)
    keys = projected[..., width:2 * width].astype(jnp.bfloat16)
    values = projected[..., 2 * width:].astype(jnp.bfloat16)
    block = math.gcd(NLON, 512)

    def one_row(operands):
        row_queries, row_keys, row_values = operands
        key_heads = row_keys.reshape(NLON, HEADS, HEAD_DIM).astype(jnp.float32)
        value_heads = row_values.reshape(NLON, HEADS, HEAD_DIM).astype(jnp.float32)
        query_blocks = row_queries.reshape(NLON // block, block, HEADS, HEAD_DIM)

        def one_block(query_block):
            scores = jnp.einsum('qhd,khd->hqk', query_block.astype(jnp.float32), key_heads)
            highest = lax.optimization_barrier(jnp.max(scores, axis=-1, keepdims=True))
            expd = jnp.exp(scores - highest)
            totals = lax.optimization_barrier(jnp.sum(expd, axis=-1))
            weights = expd.astype(jnp.bfloat16).astype(jnp.float32)
            mixed = jnp.einsum('hqk,khd->qhd', weights, value_heads)
            mixed = mixed / jnp.transpose(totals)[:, :, None]
            return mixed.reshape(block, width).astype(jnp.bfloat16)
        return lax.map(one_block, query_blocks).reshape(NLON, width)
    attended = lax.map(one_row, (queries, keys, values))
    output = jnp.dot(attended.reshape(-1, width), w_out, preferred_element_type=jnp.float32)
    return (inputs + output.reshape(NLAT, NLON, width)).astype(jnp.bfloat16)
```

```python
import math

import jax
import jax.numpy as jnp
from jax import lax
from jax.experimental import pallas as pl
from jax.experimental.pallas import tpu as pltpu
from jax.sharding import PartitionSpec as P

HEADS = 8
EPS = 1e-05
UNIT = 1024


def norm_kernel(par_ref, x_ref, gain_ref, own_ref, other_ref):
    rows = own_ref.shape[0]
    start = par_ref[0] * rows
    gain = gain_ref[...]

    def normed(row):
        x = x_ref[row].astype(jnp.float32)
        center = jnp.mean(x, axis=-1, keepdims=True)
        shifted = x - center
        spread = jnp.mean(shifted * shifted, axis=-1, keepdims=True)
        return (shifted * lax.rsqrt(spread + EPS) * gain).astype(jnp.bfloat16)

    for i in range(rows):
        other_ref[i] = normed(rows - start + i)
        own_ref[i] = normed(start + i)


def layer_norm_split(parity, fields, gain):
    rows, cells, width = fields.shape
    half = jax.ShapeDtypeStruct((rows // 2, cells, width), jnp.bfloat16)
    return pl.pallas_call(
        norm_kernel,
        out_shape=(half, half),
        in_specs=[
            pl.BlockSpec(memory_space=pltpu.SMEM),
            pl.BlockSpec(memory_space=pltpu.VMEM),
            pl.BlockSpec(memory_space=pltpu.VMEM),
        ],
        out_specs=(
            pl.BlockSpec(memory_space=pltpu.VMEM),
            pl.BlockSpec(memory_space=pltpu.VMEM),
        ),
        cost_estimate=pl.CostEstimate(flops=4_000_000, bytes_accessed=400_000, transcendentals=0),
        name="norm_split",
    )(parity, fields, gain.reshape(1, width))


def attend_rows(chunks, wk_ref, wvt_ref, q_ref, m_in, acc_in, store, s_ref, p_ref, v_ref, k_ref):
    rows, cells, width = chunks[0].shape
    head_width = width // HEADS
    count = len(chunks) * cells
    n_queries = q_ref.shape[2]
    tile = math.gcd(count, 256)
    heads = max(1, min(HEADS, UNIT // count))

    def project(r):
        x = jnp.concatenate([c[r] for c in chunks], axis=0)
        k_ref[r % 2] = jnp.dot(x, wk_ref[...], preferred_element_type=jnp.float32).astype(
            jnp.bfloat16
        )
        values_t = lax.dot_general(
            wvt_ref[...], x, (((1,), (1,)), ((), ())), preferred_element_type=jnp.float32
        ).astype(jnp.bfloat16)
        for h in range(HEADS):
            low, high = h * head_width, (h + 1) * head_width
            v_ref[r % 2, 2 * low : 2 * low + head_width, :] = values_t[low:high, :]

    def score(r, h, slot):
        low, high = h * head_width, (h + 1) * head_width
        parts = []
        if h:
            parts.append(jnp.zeros((low, n_queries), jnp.bfloat16))
        parts.append(q_ref[r, low:high, :])
        if h < HEADS - 1:
            parts.append(jnp.zeros((width - high, n_queries), jnp.bfloat16))
        q = jnp.concatenate(parts, axis=0)
        best = None
        for t in range(0, count, tile):
            s = jnp.dot(k_ref[r % 2, t : t + tile, :], q, preferred_element_type=jnp.float32)
            s_ref[slot, t : t + tile, :] = s
            top = jnp.max(s.reshape(tile // 8, 8, n_queries), axis=0)
            best = top if best is None else jnp.maximum(best, top)
        return best

    def weigh(r, h, slot, best):
        highest = jnp.max(best, axis=0, keepdims=True)
        before = None
        if m_in is not None:
            before = m_in(r, h)
            highest = jnp.maximum(highest, before)
        for t in range(0, count, tile):
            p_ref[slot, t : t + tile, :] = jnp.exp(s_ref[slot, t : t + tile, :] - highest).astype(
                jnp.bfloat16
            )
        return before, highest

    def mix(r, h, slot, before, highest):
        low, high = h * head_width, (h + 1) * head_width
        acc = jnp.dot(
            v_ref[r % 2, 2 * low : 2 * high, :], p_ref[slot], preferred_element_type=jnp.float32
        )
        if m_in is not None:
            acc = acc + acc_in(r, h) * jnp.exp(before - highest)
        store(r, h, highest, acc)

    ones = jnp.ones((head_width, count), jnp.bfloat16)
    for h in range(HEADS):
        for i in range(2):
            v_ref[i, (2 * h + 1) * head_width : 2 * (h + 1) * head_width, :] = ones
    work = [(r, h) for r in range(rows) for h in range(HEADS)]
    units = [work[i : i + heads] for i in range(0, len(work), heads)]
    project(0)

    def scores(u):
        return [score(r, h, (u % 2) * heads + i) for i, (r, h) in enumerate(units[u])]

    best = scores(0)
    for u, unit in enumerate(units):
        if unit[0][1] == 0 and unit[0][0] + 1 < rows:
            project(unit[0][0] + 1)
        following = scores(u + 1) if u + 1 < len(units) else None
        ready = [
            weigh(r, h, (u % 2) * heads + i, best[i]) for i, (r, h) in enumerate(unit)
        ]
        for i, (r, h) in enumerate(unit):
            mix(r, h, (u % 2) * heads + i, *ready[i])
        best = following


def first_kernel(n_chunks, *refs):
    chunks = refs[:n_chunks]
    wqt_ref, wk_ref, wvt_ref, q_ref, m_ref, acc_ref, *scratch = refs[n_chunks:]
    rows, cells, width = chunks[0].shape
    scale = 1.0 / math.sqrt(width // HEADS)
    for r in range(rows):
        for i in range(2):
            q = lax.dot_general(
                wqt_ref[...],
                chunks[i][r],
                (((1,), (1,)), ((), ())),
                preferred_element_type=jnp.float32,
            )
            q_ref[r, :, i * cells : (i + 1) * cells] = (q * scale).astype(jnp.bfloat16)

    def store(r, h, highest, acc):
        m_ref[r, h : h + 1, :] = highest
        acc_ref[r, h] = acc

    attend_rows(chunks, wk_ref, wvt_ref, q_ref, None, None, store, *scratch)


def middle_kernel(n_chunks, *refs):
    chunks = refs[:n_chunks]
    wk_ref, wvt_ref, q_ref, m_in, acc_in, m_ref, acc_ref, *scratch = refs[n_chunks:]

    def store(r, h, highest, acc):
        m_ref[r, h : h + 1, :] = highest
        acc_ref[r, h] = acc

    attend_rows(
        chunks,
        wk_ref,
        wvt_ref,
        q_ref,
        lambda r, h: m_in[r, h : h + 1, :],
        lambda r, h: acc_in[r, h],
        store,
        *scratch,
    )


def last_kernel(n_chunks, *refs):
    chunks = refs[:n_chunks]
    wk_ref, wvt_ref, q_ref, m_in, acc_in, own_ref, other_ref, *scratch = refs[n_chunks:]
    head_width = wk_ref.shape[0] // HEADS
    cells = own_ref.shape[2]

    def store(r, h, highest, acc):
        low, high = h * head_width, (h + 1) * head_width
        mixed = (acc[:head_width] / acc[head_width : head_width + 1]).astype(jnp.bfloat16)
        own_ref[r, low:high, :] = mixed[:, :cells]
        other_ref[r, low:high, :] = mixed[:, cells:]

    attend_rows(
        chunks,
        wk_ref,
        wvt_ref,
        q_ref,
        lambda r, h: m_in[r, h : h + 1, :],
        lambda r, h: acc_in[r, h],
        store,
        *scratch,
    )


def attend(kind, chunks, weights, state):
    rows, cells, width = chunks[0].shape
    n = len(chunks)
    head_width = width // HEADS
    q_shape = jax.ShapeDtypeStruct((rows, width, 2 * cells), jnp.bfloat16)
    m_shape = jax.ShapeDtypeStruct((rows, HEADS, 2 * cells), jnp.float32)
    acc_shape = jax.ShapeDtypeStruct((rows, HEADS, 2 * head_width, 2 * cells), jnp.float32)
    half = jax.ShapeDtypeStruct((rows, width, cells), jnp.bfloat16)
    kernel, outs = {
        "first": (first_kernel, (q_shape, m_shape, acc_shape)),
        "middle": (middle_kernel, (m_shape, acc_shape)),
        "last": (last_kernel, (half, half)),
    }[kind]
    scores = rows * HEADS * n * cells * 2 * cells
    operands = [*chunks, *weights, *state]
    heads = max(1, min(HEADS, UNIT // (n * cells)))
    vmem = pl.BlockSpec(memory_space=pltpu.VMEM)

    def body(*refs):
        kernel(n, *refs)

    return pl.pallas_call(
        body,
        in_specs=[vmem] * len(operands),
        out_specs=(vmem,) * len(outs),
        out_shape=outs,
        scratch_shapes=[
            pltpu.VMEM((2 * heads, n * cells, 2 * cells), jnp.float32),
            pltpu.VMEM((2 * heads, n * cells, 2 * cells), jnp.bfloat16),
            pltpu.VMEM((2, 2 * width, n * cells), jnp.bfloat16),
            pltpu.VMEM((2, n * cells, width), jnp.bfloat16),
        ],
        cost_estimate=pl.CostEstimate(
            flops=scores * 2 * 160, bytes_accessed=1_000_000, transcendentals=scores
        ),
        name="attend_" + kind,
    )(*operands)


def out_kernel(par_ref, x_ref, own_ref, other_ref, w_ref, o_ref):
    rows = own_ref.shape[0]
    start = par_ref[0] * rows
    w = w_ref[...]

    def project(attended_t, row):
        y = lax.dot_general(
            attended_t, w, (((0,), (0,)), ((), ())), preferred_element_type=jnp.float32
        )
        o_ref[row] = (x_ref[row].astype(jnp.float32) + y).astype(jnp.bfloat16)

    for i in range(rows):
        project(own_ref[i], start + i)
        project(other_ref[i], rows - start + i)


def project_out(parity, fields, own, other, w_out):
    vmem = pl.BlockSpec(memory_space=pltpu.VMEM)
    return pl.pallas_call(
        out_kernel,
        out_shape=jax.ShapeDtypeStruct(fields.shape, fields.dtype),
        in_specs=[pl.BlockSpec(memory_space=pltpu.SMEM), vmem, vmem, vmem, vmem],
        out_specs=vmem,
        cost_estimate=pl.CostEstimate(flops=25_000_000, bytes_accessed=600_000, transcendentals=0),
        name="project_out",
    )(parity, fields, own, other, w_out)


def body(fields, norm_gain, w_qkv, w_out):
    size = lax.axis_size("lon")
    width = fields.shape[2]
    position = lax.axis_index("lon")
    parity = (position % 2).astype(jnp.int32).reshape(1)

    def shift(block, by):
        return lax.ppermute(block, "lon", [(i, (i + by) % size) for i in range(size)])

    def swap(block):
        return lax.ppermute(block, "lon", [(i, i ^ 1) for i in range(size)])

    wqt = w_qkv[:, :width].T
    wk = w_qkv[:, width : 2 * width]
    wvt = w_qkv[:, 2 * width :].T

    own, other = layer_norm_split(parity, fields, norm_gain)
    partner = swap(other)
    a_up = a_down = own
    b_up = b_down = partner
    ring = size // 2
    groups = []
    for _ in range((ring - 1) // 2):
        a_up, a_down = shift(a_up, 2), shift(a_down, -2)
        b_up, b_down = shift(b_up, 2), shift(b_down, -2)
        groups.append([a_up, a_down, b_up, b_down])
    if ring % 2 == 0:
        groups.append([shift(a_up, 2), shift(b_down, -2)])
    groups[0] = [own, partner] + groups[0]

    q, m, acc = attend("first", groups[0], (wqt, wk, wvt), ())
    for group in groups[1:-1]:
        m, acc = attend("middle", group, (wk, wvt), (q, m, acc))
    mine, theirs = attend("last", groups[-1], (wk, wvt), (q, m, acc))
    back = swap(theirs)
    return project_out(parity, fields, mine, back, w_out)


def solution(mesh):
    return jax.shard_map(
        body,
        mesh=mesh,
        in_specs=(P(("groups", "lat"), "lon", None), P(), P(), P()),
        out_specs=P(("groups", "lat"), "lon", None),
        check_vma=False,
    )
```

```python
import math

import jax
import jax.numpy as jnp
from jax import lax
from jax.experimental import pallas as pl
from jax.experimental.pallas import tpu as pltpu
from jax.sharding import PartitionSpec as P

HEADS = 8
EPS = 1e-05
UNIT = 1024
SMALL = 6 * 2**20
LARGE = 20 * 2**20


def norm_kernel(par_ref, x_hbm, gain_hbm, own_ref, other_ref, x_ref, gain_ref, sems):
    copies = [
        pltpu.make_async_copy(x_hbm, x_ref, sems.at[0]),
        pltpu.make_async_copy(gain_hbm, gain_ref, sems.at[1]),
    ]
    for copy in copies:
        copy.start()
    for copy in copies:
        copy.wait()
    rows = own_ref.shape[0]
    start = par_ref[0] * rows
    gain = gain_ref[...]

    def normed(row):
        x = x_ref[row].astype(jnp.float32)
        center = jnp.mean(x, axis=-1, keepdims=True)
        shifted = x - center
        spread = jnp.mean(shifted * shifted, axis=-1, keepdims=True)
        return (shifted * lax.rsqrt(spread + EPS) * gain).astype(jnp.bfloat16)

    for i in range(rows):
        other_ref[i] = normed(rows - start + i)
        own_ref[i] = normed(start + i)


def layer_norm_split(parity, fields, gain):
    rows, cells, width = fields.shape
    half = jax.ShapeDtypeStruct((rows // 2, cells, width), jnp.bfloat16)
    vmem = pl.BlockSpec(memory_space=pltpu.VMEM)
    hbm = pl.BlockSpec(memory_space=pltpu.HBM)
    return pl.pallas_call(
        norm_kernel,
        out_shape=(half, half),
        in_specs=[pl.BlockSpec(memory_space=pltpu.SMEM), hbm, hbm],
        out_specs=(vmem, vmem),
        scratch_shapes=[
            pltpu.VMEM(fields.shape, fields.dtype),
            pltpu.VMEM((1, width), jnp.float32),
            pltpu.SemaphoreType.DMA((2,)),
        ],
        compiler_params=pltpu.CompilerParams(vmem_limit_bytes=SMALL),
        cost_estimate=pl.CostEstimate(flops=4_000_000, bytes_accessed=400_000, transcendentals=0),
        name="norm_split",
    )(parity, fields, gain.reshape(1, width))


def attend_rows(chunks, w_ref, wt_ref, q_ref, m_in, acc_in, store, s_ref, p_ref, v_ref, k_ref):
    rows, cells, width = chunks[0].shape
    head_width = width // HEADS
    count = len(chunks) * cells
    n_queries = q_ref.shape[2]
    tile = math.gcd(count, 256)
    heads = max(1, min(HEADS, UNIT // count))

    def project(r):
        x = jnp.concatenate([c[r] for c in chunks], axis=0)
        k_ref[r % 2] = jnp.dot(x, w_ref[:, width : 2 * width], preferred_element_type=jnp.float32).astype(
            jnp.bfloat16
        )
        values_t = lax.dot_general(
            wt_ref[2 * width :, :], x, (((1,), (1,)), ((), ())), preferred_element_type=jnp.float32
        ).astype(jnp.bfloat16)
        for h in range(HEADS):
            low, high = h * head_width, (h + 1) * head_width
            v_ref[r % 2, 2 * low : 2 * low + head_width, :] = values_t[low:high, :]

    def score(r, h, slot):
        low, high = h * head_width, (h + 1) * head_width
        parts = []
        if h:
            parts.append(jnp.zeros((low, n_queries), jnp.bfloat16))
        parts.append(q_ref[r, low:high, :])
        if h < HEADS - 1:
            parts.append(jnp.zeros((width - high, n_queries), jnp.bfloat16))
        q = jnp.concatenate(parts, axis=0)
        best = None
        for t in range(0, count, tile):
            s = jnp.dot(k_ref[r % 2, t : t + tile, :], q, preferred_element_type=jnp.float32)
            s_ref[slot, t : t + tile, :] = s
            top = jnp.max(s.reshape(tile // 8, 8, n_queries), axis=0)
            best = top if best is None else jnp.maximum(best, top)
        return best

    def weigh(r, h, slot, best):
        highest = jnp.max(best, axis=0, keepdims=True)
        before = None
        if m_in is not None:
            before = m_in(r, h)
            highest = jnp.maximum(highest, before)
        for t in range(0, count, tile):
            p_ref[slot, t : t + tile, :] = jnp.exp(s_ref[slot, t : t + tile, :] - highest).astype(
                jnp.bfloat16
            )
        return before, highest

    def mix(r, h, slot, before, highest):
        low, high = h * head_width, (h + 1) * head_width
        acc = jnp.dot(
            v_ref[r % 2, 2 * low : 2 * high, :], p_ref[slot], preferred_element_type=jnp.float32
        )
        if m_in is not None:
            acc = acc + acc_in(r, h) * jnp.exp(before - highest)
        store(r, h, highest, acc)

    ones = jnp.ones((head_width, count), jnp.bfloat16)
    for h in range(HEADS):
        for i in range(2):
            v_ref[i, (2 * h + 1) * head_width : 2 * (h + 1) * head_width, :] = ones
    work = [(r, h) for r in range(rows) for h in range(HEADS)]
    units = [work[i : i + heads] for i in range(0, len(work), heads)]
    project(0)

    def scores(u):
        return [score(r, h, (u % 2) * heads + i) for i, (r, h) in enumerate(units[u])]

    best = scores(0)
    for u, unit in enumerate(units):
        if unit[0][1] == 0 and unit[0][0] + 1 < rows:
            project(unit[0][0] + 1)
        following = scores(u + 1) if u + 1 < len(units) else None
        ready = [
            weigh(r, h, (u % 2) * heads + i, best[i]) for i, (r, h) in enumerate(unit)
        ]
        for i, (r, h) in enumerate(unit):
            mix(r, h, (u % 2) * heads + i, *ready[i])
        best = following


def first_kernel(n_chunks, *refs):
    chunks = refs[:n_chunks]
    w_ref, q_ref, wt_ref, m_ref, acc_ref, *scratch = refs[n_chunks:]
    rows, cells, width = chunks[0].shape
    scale = 1.0 / math.sqrt(width // HEADS)
    wt_ref[...] = w_ref[...].T
    for r in range(rows):
        for i in range(2):
            q = lax.dot_general(
                wt_ref[:width, :],
                chunks[i][r],
                (((1,), (1,)), ((), ())),
                preferred_element_type=jnp.float32,
            )
            q_ref[r, :, i * cells : (i + 1) * cells] = (q * scale).astype(jnp.bfloat16)

    def store(r, h, highest, acc):
        m_ref[r, h : h + 1, :] = highest
        acc_ref[r, h] = acc

    attend_rows(chunks, w_ref, wt_ref, q_ref, None, None, store, *scratch)


def middle_kernel(n_chunks, *refs):
    chunks = refs[:n_chunks]
    w_ref, wt_ref, q_ref, m_in, acc_in, m_ref, acc_ref, *scratch = refs[n_chunks:]

    def store(r, h, highest, acc):
        m_ref[r, h : h + 1, :] = highest
        acc_ref[r, h] = acc

    attend_rows(
        chunks,
        w_ref,
        wt_ref,
        q_ref,
        lambda r, h: m_in[r, h : h + 1, :],
        lambda r, h: acc_in[r, h],
        store,
        *scratch,
    )


def last_kernel(n_chunks, *refs):
    chunks = refs[:n_chunks]
    w_ref, wt_ref, q_ref, m_in, acc_in, own_ref, other_ref, *scratch = refs[n_chunks:]
    head_width = w_ref.shape[0] // HEADS
    cells = own_ref.shape[2]

    def store(r, h, highest, acc):
        low, high = h * head_width, (h + 1) * head_width
        mixed = (acc[:head_width] / acc[head_width : head_width + 1]).astype(jnp.bfloat16)
        own_ref[r, low:high, :] = mixed[:, :cells]
        other_ref[r, low:high, :] = mixed[:, cells:]

    attend_rows(
        chunks,
        w_ref,
        wt_ref,
        q_ref,
        lambda r, h: m_in[r, h : h + 1, :],
        lambda r, h: acc_in[r, h],
        store,
        *scratch,
    )


def attend(kind, chunks, weights, state):
    rows, cells, width = chunks[0].shape
    n = len(chunks)
    head_width = width // HEADS
    q_shape = jax.ShapeDtypeStruct((rows, width, 2 * cells), jnp.bfloat16)
    wt_shape = jax.ShapeDtypeStruct((3 * width, width), jnp.bfloat16)
    m_shape = jax.ShapeDtypeStruct((rows, HEADS, 2 * cells), jnp.float32)
    acc_shape = jax.ShapeDtypeStruct((rows, HEADS, 2 * head_width, 2 * cells), jnp.float32)
    half = jax.ShapeDtypeStruct((rows, width, cells), jnp.bfloat16)
    kernel, outs = {
        "first": (first_kernel, (q_shape, wt_shape, m_shape, acc_shape)),
        "middle": (middle_kernel, (m_shape, acc_shape)),
        "last": (last_kernel, (half, half)),
    }[kind]
    scores = rows * HEADS * n * cells * 2 * cells
    operands = [*chunks, *weights, *state]
    heads = max(1, min(HEADS, UNIT // (n * cells)))
    vmem = pl.BlockSpec(memory_space=pltpu.VMEM)

    def body(*refs):
        kernel(n, *refs)

    return pl.pallas_call(
        body,
        in_specs=[vmem] * len(operands),
        out_specs=(vmem,) * len(outs),
        out_shape=outs,
        scratch_shapes=[
            pltpu.VMEM((2 * heads, n * cells, 2 * cells), jnp.float32),
            pltpu.VMEM((2 * heads, n * cells, 2 * cells), jnp.bfloat16),
            pltpu.VMEM((2, 2 * width, n * cells), jnp.bfloat16),
            pltpu.VMEM((2, n * cells, width), jnp.bfloat16),
        ],
        compiler_params=pltpu.CompilerParams(vmem_limit_bytes=LARGE),
        cost_estimate=pl.CostEstimate(
            flops=scores * 2 * 160, bytes_accessed=1_000_000, transcendentals=scores
        ),
        name="attend_" + kind,
    )(*operands)


def out_kernel(par_ref, x_ref, own_ref, other_ref, w_ref, o_ref):
    rows = own_ref.shape[0]
    start = par_ref[0] * rows
    w = w_ref[...]

    def project(attended_t, row):
        y = lax.dot_general(
            attended_t, w, (((0,), (0,)), ((), ())), preferred_element_type=jnp.float32
        )
        o_ref[row] = (x_ref[row].astype(jnp.float32) + y).astype(jnp.bfloat16)

    for i in range(rows):
        project(own_ref[i], start + i)
        project(other_ref[i], rows - start + i)


def project_out(parity, fields, own, other, w_out):
    vmem = pl.BlockSpec(memory_space=pltpu.VMEM)
    return pl.pallas_call(
        out_kernel,
        out_shape=jax.ShapeDtypeStruct(fields.shape, fields.dtype),
        in_specs=[pl.BlockSpec(memory_space=pltpu.SMEM), vmem, vmem, vmem, vmem],
        out_specs=vmem,
        compiler_params=pltpu.CompilerParams(vmem_limit_bytes=SMALL),
        cost_estimate=pl.CostEstimate(flops=25_000_000, bytes_accessed=600_000, transcendentals=0),
        name="project_out",
    )(parity, fields, own, other, w_out)


def body(fields, norm_gain, w_qkv, w_out):
    size = lax.axis_size("lon")
    width = fields.shape[2]
    position = lax.axis_index("lon")
    parity = (position % 2).astype(jnp.int32).reshape(1)

    def shift(block, by):
        return lax.ppermute(block, "lon", [(i, (i + by) % size) for i in range(size)])

    def swap(block):
        return lax.ppermute(block, "lon", [(i, i ^ 1) for i in range(size)])

    own, other = layer_norm_split(parity, fields, norm_gain)
    partner = swap(other)
    a_blocks, b_blocks = [own], [partner]
    ring = size // 2
    a_up = a_down = own
    b_up = b_down = partner
    q = wt = state = None
    for step in range(1, ring // 2 + 1):
        if state is not None:
            a_up, a_down, state = lax.optimization_barrier((a_up, a_down, state))
        if 2 * step < ring:
            next_a = [shift(a_up, 2), shift(a_down, -2)]
            next_b = [shift(b_up, 2), shift(b_down, -2)]
        else:
            next_a, next_b = [shift(a_up, 2)], [shift(b_down, -2)]
        if state is None:
            q, wt, *state = attend("first", a_blocks + b_blocks, (w_qkv,), ())
        else:
            state = attend("middle", a_blocks + b_blocks, (w_qkv, wt), (q, *state))
        state = tuple(state)
        a_blocks, b_blocks = next_a, next_b
        a_up, a_down = next_a[0], next_a[-1]
        b_up, b_down = next_b[0], next_b[-1]
    mine, theirs = attend("last", a_blocks + b_blocks, (w_qkv, wt), (q, *state))
    back = swap(theirs)
    return project_out(parity, fields, mine, back, w_out)


def solution(mesh):
    return jax.shard_map(
        body,
        mesh=mesh,
        in_specs=(P(("groups", "lat"), "lon", None), P(), P(), P()),
        out_specs=P(("groups", "lat"), "lon", None),
        check_vma=False,
    )
```

```python
import math

import jax
import jax.numpy as jnp
from jax import lax
from jax.experimental import pallas as pl
from jax.experimental.pallas import tpu as pltpu
from jax.sharding import PartitionSpec as P

HEADS = 8
EPS = 1e-05
LOG2E = math.log2(math.e)
UNIT = 1024
SMALL = 6 * 2**20
LARGE = 20 * 2**20


def norm_kernel(par_ref, x_ref, gain_ref, own_ref, other_ref):
    rows = own_ref.shape[0]
    start = par_ref[0] * rows
    gain = gain_ref[...]

    def normed(row):
        x = x_ref[row].astype(jnp.float32)
        center = jnp.mean(x, axis=-1, keepdims=True)
        shifted = x - center
        spread = jnp.mean(shifted * shifted, axis=-1, keepdims=True)
        return (shifted * lax.rsqrt(spread + EPS) * gain).astype(jnp.bfloat16)

    for i in range(rows):
        other_ref[i] = normed(rows - start + i)
        own_ref[i] = normed(start + i)


def layer_norm_split(parity, fields, gain):
    rows, cells, width = fields.shape
    half = jax.ShapeDtypeStruct((rows // 2, cells, width), jnp.bfloat16)
    vmem = pl.BlockSpec(memory_space=pltpu.VMEM)
    return pl.pallas_call(
        norm_kernel,
        out_shape=(half, half),
        in_specs=[pl.BlockSpec(memory_space=pltpu.SMEM), vmem, vmem],
        out_specs=(vmem, vmem),
        compiler_params=pltpu.CompilerParams(vmem_limit_bytes=SMALL),
        cost_estimate=pl.CostEstimate(flops=4_000_000, bytes_accessed=400_000, transcendentals=0),
        name="norm_split",
    )(parity, fields, gain.reshape(1, width))


def attend_rows(chunks, w_ref, wt_ref, q_ref, lanes, m_in, acc_in, store, s_ref, p_ref, v_ref, k_ref):
    rows, cells, width = chunks[0].shape
    head_width = width // HEADS
    count = len(chunks) * cells
    n_queries = lanes.stop - lanes.start
    tile = 256 if count % 256 == 0 else count
    heads = max(1, min(HEADS, UNIT // count))

    def project(r):
        x = jnp.concatenate([c[r] for c in chunks], axis=0)
        keys = jnp.dot(
            x, w_ref[:, width : 2 * width], preferred_element_type=jnp.float32
        ).astype(jnp.bfloat16)
        k_ref[r % 2, :, :width] = keys
        k_ref[r % 2, :, width:] = keys
        values_t = lax.dot_general(
            wt_ref[2 * width :, :], x, (((1,), (1,)), ((), ())), preferred_element_type=jnp.float32
        ).astype(jnp.bfloat16)
        for h in range(HEADS):
            low, high = h * head_width, (h + 1) * head_width
            v_ref[r % 2, 2 * low : 2 * low + head_width, :] = values_t[low:high, :]

    def score(r, h, slot):
        low, high = h * head_width, (h + 1) * head_width
        parts = []
        for half in range(2):
            if h:
                parts.append(jnp.zeros((low, n_queries), jnp.bfloat16))
            parts.append(q_ref[r, half * width + low : half * width + high, lanes])
            if h < HEADS - 1:
                parts.append(jnp.zeros((width - high, n_queries), jnp.bfloat16))
        q = jnp.concatenate(parts, axis=0)
        best = None
        for t in range(0, count, tile):
            s = jnp.dot(k_ref[r % 2, t : t + tile, :], q, preferred_element_type=jnp.float32)
            s_ref[slot, t : t + tile, :] = s
            top = jnp.max(s.reshape(tile // 8, 8, n_queries), axis=0)
            best = top if best is None else jnp.maximum(best, top)
        return best

    def weigh(r, h, slot, best):
        highest = jnp.max(best, axis=0, keepdims=True)
        before = None
        if m_in is not None:
            before = m_in(r, h)
            highest = jnp.maximum(highest, before)
        for t in range(0, count, tile):
            p_ref[slot, t : t + tile, :] = jnp.exp2(s_ref[slot, t : t + tile, :] - highest).astype(
                jnp.bfloat16
            )
        return before, highest

    def mix(r, h, slot, before, highest):
        low, high = h * head_width, (h + 1) * head_width
        acc = jnp.dot(
            v_ref[r % 2, 2 * low : 2 * high, :], p_ref[slot], preferred_element_type=jnp.float32
        )
        if m_in is not None:
            acc = acc + acc_in(r, h) * jnp.exp2(before - highest)
        store(r, h, highest, acc)

    ones = jnp.ones((head_width, count), jnp.bfloat16)
    for h in range(HEADS):
        for i in range(2):
            v_ref[i, (2 * h + 1) * head_width : 2 * (h + 1) * head_width, :] = ones
    work = [(r, h) for r in range(rows) for h in range(HEADS)]
    units = [work[i : i + heads] for i in range(0, len(work), heads)]
    project(0)

    def scores(u):
        return [score(r, h, (u % 2) * heads + i) for i, (r, h) in enumerate(units[u])]

    best = scores(0)
    for u, unit in enumerate(units):
        if unit[0][1] == 0 and unit[0][0] + 1 < rows:
            project(unit[0][0] + 1)
        following = scores(u + 1) if u + 1 < len(units) else None
        ready = [
            weigh(r, h, (u % 2) * heads + i, best[i]) for i, (r, h) in enumerate(unit)
        ]
        for i, (r, h) in enumerate(unit):
            mix(r, h, (u % 2) * heads + i, *ready[i])
        best = following


def first_kernel(n_chunks, par_ref, *refs):
    chunks = refs[:n_chunks]
    w_ref, q_ref, wt_ref, m_ref, acc_ref, *scratch = refs[n_chunks:]
    rows, cells, width = chunks[0].shape
    scale = 1.0 / math.sqrt(width // HEADS)
    wt_ref[...] = w_ref[...].T
    upper = par_ref[0] == 0
    for r in range(rows):
        for i, x in enumerate([chunks[0][r], jnp.where(upper, chunks[2][r], chunks[1][r])]):
            q = lax.dot_general(
                wt_ref[:width, :], x, (((1,), (1,)), ((), ())), preferred_element_type=jnp.float32
            )
            q = (q * scale).astype(jnp.bfloat16).astype(jnp.float32) * LOG2E
            high = q.astype(jnp.bfloat16)
            q_ref[r, :width, i * cells : (i + 1) * cells] = high
            q_ref[r, width:, i * cells : (i + 1) * cells] = (
                q - high.astype(jnp.float32)
            ).astype(jnp.bfloat16)

    def store(r, h, highest, acc):
        m_ref[r, h : h + 1, :] = highest
        acc_ref[r, h] = acc

    attend_rows(
        chunks, w_ref, wt_ref, q_ref, slice(0, 2 * cells), None, None, store, *scratch
    )


def middle_kernel(n_chunks, *refs):
    chunks = refs[:n_chunks]
    w_ref, wt_ref, q_ref, m_in, acc_in, m_ref, acc_ref, *scratch = refs[n_chunks:]

    def store(r, h, highest, acc):
        m_ref[r, h : h + 1, :] = highest
        acc_ref[r, h] = acc

    attend_rows(
        chunks,
        w_ref,
        wt_ref,
        q_ref,
        slice(0, q_ref.shape[2]),
        lambda r, h: m_in[r, h : h + 1, :],
        lambda r, h: acc_in[r, h],
        store,
        *scratch,
    )


def finish(chunks, w_ref, wt_ref, q_ref, m_in, acc_in, lanes, out_ref, scratch):
    head_width = w_ref.shape[0] // HEADS

    def store(r, h, highest, acc):
        mixed = acc[:head_width] / acc[head_width : head_width + 1]
        out_ref[r, h * head_width : (h + 1) * head_width, :] = mixed.astype(jnp.bfloat16)

    attend_rows(
        chunks,
        w_ref,
        wt_ref,
        q_ref,
        lanes,
        lambda r, h: m_in[r, h : h + 1, lanes],
        lambda r, h: acc_in[r, h, :, lanes],
        store,
        *scratch,
    )


def project(attended_t, w, x):
    y = lax.dot_general(attended_t, w, (((0,), (0,)), ((), ())), preferred_element_type=jnp.float32)
    return (x.astype(jnp.float32) + y).astype(jnp.bfloat16)


def theirs_kernel(n_chunks, *refs):
    *operands, out_ref = refs[n_chunks : n_chunks + 6]
    cells = out_ref.shape[2]
    finish(refs[:n_chunks], *operands, slice(cells, 2 * cells), out_ref, refs[n_chunks + 6 :])


def mine_kernel(n_chunks, par_ref, *refs):
    *operands, x_ref, wo_ref, out_ref = refs[n_chunks : n_chunks + 8]
    *scratch, mixed_ref = refs[n_chunks + 8 :]
    rows, cells, _ = out_ref.shape
    finish(refs[:n_chunks], *operands, slice(0, cells), mixed_ref, scratch)
    for i in range(rows):
        out_ref[i] = project(mixed_ref[i], wo_ref[...], x_ref[par_ref[0] * rows + i])


def attend(kind, chunks, weights, state, parity=None):
    rows, cells, width = chunks[0].shape
    n = len(chunks)
    head_width = width // HEADS
    q_shape = jax.ShapeDtypeStruct((rows, 2 * width, 2 * cells), jnp.bfloat16)
    wt_shape = jax.ShapeDtypeStruct((3 * width, width), jnp.bfloat16)
    m_shape = jax.ShapeDtypeStruct((rows, HEADS, 2 * cells), jnp.float32)
    acc_shape = jax.ShapeDtypeStruct((rows, HEADS, 2 * head_width, 2 * cells), jnp.float32)
    half = jax.ShapeDtypeStruct((rows, width, cells), jnp.bfloat16)
    kernel, outs = {
        "first": (first_kernel, (q_shape, wt_shape, m_shape, acc_shape)),
        "middle": (middle_kernel, (m_shape, acc_shape)),
        "theirs": (theirs_kernel, (half,)),
        "mine": (mine_kernel, (jax.ShapeDtypeStruct((rows, cells, width), jnp.bfloat16),)),
    }[kind]
    scores = rows * HEADS * n * cells * 2 * cells
    operands = [*chunks, *weights, *state]
    heads = max(1, min(HEADS, UNIT // (n * cells)))
    n_queries = 2 * cells if kind in ("first", "middle") else cells
    vmem = pl.BlockSpec(memory_space=pltpu.VMEM)

    scratch = [
        pltpu.VMEM((2 * heads, n * cells, n_queries), jnp.float32),
        pltpu.VMEM((2 * heads, n * cells, n_queries), jnp.bfloat16),
        pltpu.VMEM((2, 2 * width, n * cells), jnp.bfloat16),
        pltpu.VMEM((2, n * cells, 2 * width), jnp.bfloat16),
    ]
    if kind == "mine":
        scratch.append(pltpu.VMEM(half.shape, half.dtype))

    def body(*refs):
        kernel(n, *refs)

    in_specs = [vmem] * len(operands)
    if parity is not None:
        operands.insert(0, parity)
        in_specs.insert(0, pl.BlockSpec(memory_space=pltpu.SMEM))

    return pl.pallas_call(
        body,
        in_specs=in_specs,
        out_specs=(vmem,) * len(outs),
        out_shape=outs,
        scratch_shapes=scratch,
        compiler_params=pltpu.CompilerParams(vmem_limit_bytes=LARGE),
        cost_estimate=pl.CostEstimate(
            flops=scores * 2 * 160 * n_queries // (2 * cells), bytes_accessed=1_000_000, transcendentals=scores
        ),
        name="attend_" + kind,
    )(*operands)


def out_kernel(par_ref, x_ref, done_ref, other_ref, w_ref, o_ref):
    rows = done_ref.shape[0]
    start = par_ref[0] * rows
    for i in range(rows):
        o_ref[start + i] = done_ref[i]
        o_ref[rows - start + i] = project(other_ref[i], w_ref[...], x_ref[rows - start + i])


def project_out(parity, fields, done, other, w_out):
    vmem = pl.BlockSpec(memory_space=pltpu.VMEM)
    return pl.pallas_call(
        out_kernel,
        out_shape=jax.ShapeDtypeStruct(fields.shape, fields.dtype),
        in_specs=[pl.BlockSpec(memory_space=pltpu.SMEM), vmem, vmem, vmem, vmem],
        out_specs=vmem,
        compiler_params=pltpu.CompilerParams(vmem_limit_bytes=SMALL),
        cost_estimate=pl.CostEstimate(flops=12_000_000, bytes_accessed=600_000, transcendentals=0),
        name="project_out",
    )(parity, fields, done, other, w_out)


def body(fields, norm_gain, w_qkv, w_out):
    size = lax.axis_size("lon")
    width = fields.shape[2]
    position = lax.axis_index("lon")
    parity = (position % 2).astype(jnp.int32).reshape(1)

    def shift(block, by):
        return lax.ppermute(block, "lon", [(i, (i + by) % size) for i in range(size)])

    def swap(block):
        return lax.ppermute(block, "lon", [(i, i ^ 1) for i in range(size)])

    own, other = layer_norm_split(parity, fields, norm_gain)
    levels = size // 4
    b = [shift(other, 1), shift(other, -1)]
    a = [shift(own, 2), shift(own, -2)]
    first = [own, *b]
    b = [shift(b[0], 2), shift(b[1], -2)]
    q, wt, *state = attend("first", first, (w_qkv,), (), parity)
    for level in range(1, levels):
        a, state = lax.optimization_barrier((a, state))
        chunks = a + b
        a = [shift(a[0], 2), shift(a[1], -2)] if level < levels - 1 else [shift(a[1], -2)]
        b = [shift(b[0], 2), shift(b[1], -2)] if level < levels - 1 else []
        state = attend("middle", chunks, (w_qkv, wt), (q, *state))
    (theirs,) = attend("theirs", a, (w_qkv, wt), (q, *state))
    back = swap(theirs)
    (mine,) = attend("mine", a, (w_qkv, wt), (q, *state, fields, w_out), parity)
    return project_out(parity, fields, mine, back, w_out)


def solution(mesh):
    return jax.shard_map(
        body,
        mesh=mesh,
        in_specs=(P(("groups", "lat"), "lon", None), P(), P(), P()),
        out_specs=P(("groups", "lat"), "lon", None),
        check_vma=False,
    )
```

```python
import math

import jax
import jax.numpy as jnp
from jax import lax
from jax.experimental import pallas as pl
from jax.experimental.pallas import tpu as pltpu
from jax.sharding import PartitionSpec as P

HEADS = 8
EPS = 1e-05
LOG2E = math.log2(math.e)
UNIT = 1024
SMALL = 6 * 2**20
LARGE = 20 * 2**20


def norm_kernel(par_ref, x_ref, gain_ref, own_ref, other_ref):
    rows = own_ref.shape[0]
    start = par_ref[0] * rows
    gain = gain_ref[...]

    def normed(row):
        x = x_ref[row].astype(jnp.float32)
        center = jnp.mean(x, axis=-1, keepdims=True)
        shifted = x - center
        spread = jnp.mean(shifted * shifted, axis=-1, keepdims=True)
        return (shifted * lax.rsqrt(spread + EPS) * gain).astype(jnp.bfloat16)

    for i in range(rows):
        other_ref[i] = normed(rows - start + i)
        own_ref[i] = normed(start + i)


def layer_norm_split(parity, fields, gain):
    rows, cells, width = fields.shape
    half = jax.ShapeDtypeStruct((rows // 2, cells, width), jnp.bfloat16)
    vmem = pl.BlockSpec(memory_space=pltpu.VMEM)
    return pl.pallas_call(
        norm_kernel,
        out_shape=(half, half),
        in_specs=[pl.BlockSpec(memory_space=pltpu.SMEM), vmem, vmem],
        out_specs=(vmem, vmem),
        compiler_params=pltpu.CompilerParams(vmem_limit_bytes=SMALL),
        cost_estimate=pl.CostEstimate(flops=4_000_000, bytes_accessed=400_000, transcendentals=0),
        name="norm_split",
    )(parity, fields, gain.reshape(1, width))


def attend_rows(chunks, w_ref, wt_ref, q_ref, lanes, m_in, acc_in, store, s_ref, p_ref, v_ref, k_ref):
    rows, cells, width = chunks[0].shape
    head_width = width // HEADS
    count = len(chunks) * cells
    n_queries = lanes.stop - lanes.start
    tile = 256 if count % 256 == 0 else count
    heads = max(1, min(HEADS, UNIT // count))

    def project(r):
        x = jnp.concatenate([c[r] for c in chunks], axis=0)
        keys = jnp.dot(
            x, w_ref[:, width : 2 * width], preferred_element_type=jnp.float32
        ).astype(jnp.bfloat16)
        k_ref[r % 2, :, :width] = keys
        k_ref[r % 2, :, width:] = keys
        values_t = lax.dot_general(
            wt_ref[2 * width :, :], x, (((1,), (1,)), ((), ())), preferred_element_type=jnp.float32
        ).astype(jnp.bfloat16)
        for h in range(HEADS):
            low, high = h * head_width, (h + 1) * head_width
            v_ref[r % 2, 2 * low : 2 * low + head_width, :] = values_t[low:high, :]

    def score(r, h, slot):
        low, high = h * head_width, (h + 1) * head_width
        parts = []
        for half in range(2):
            if h:
                parts.append(jnp.zeros((low, n_queries), jnp.bfloat16))
            parts.append(q_ref[r, half * width + low : half * width + high, lanes])
            if h < HEADS - 1:
                parts.append(jnp.zeros((width - high, n_queries), jnp.bfloat16))
        q = jnp.concatenate(parts, axis=0)
        best = None
        for t in range(0, count, tile):
            s = jnp.dot(k_ref[r % 2, t : t + tile, :], q, preferred_element_type=jnp.float32)
            s_ref[slot, t : t + tile, :] = s
            top = jnp.max(s.reshape(tile // 8, 8, n_queries), axis=0)
            best = top if best is None else jnp.maximum(best, top)
        return best

    def weigh(r, h, slot, best):
        highest = jnp.max(best, axis=0, keepdims=True)
        before = None
        if m_in is not None:
            before = m_in(r, h)
            highest = jnp.maximum(highest, before)
        for t in range(0, count, tile):
            p_ref[slot, t : t + tile, :] = jnp.exp2(s_ref[slot, t : t + tile, :] - highest).astype(
                jnp.bfloat16
            )
        return before, highest

    def mix(r, h, slot, before, highest):
        low, high = h * head_width, (h + 1) * head_width
        acc = jnp.dot(
            v_ref[r % 2, 2 * low : 2 * high, :], p_ref[slot], preferred_element_type=jnp.float32
        )
        if m_in is not None:
            acc = acc + acc_in(r, h) * jnp.exp2(before - highest)
        store(r, h, highest, acc)

    ones = jnp.ones((head_width, count), jnp.bfloat16)
    for h in range(HEADS):
        for i in range(2):
            v_ref[i, (2 * h + 1) * head_width : 2 * (h + 1) * head_width, :] = ones
    work = [(r, h) for r in range(rows) for h in range(HEADS)]
    units = [work[i : i + heads] for i in range(0, len(work), heads)]
    project(0)

    def scores(u):
        return [score(r, h, (u % 2) * heads + i) for i, (r, h) in enumerate(units[u])]

    best = scores(0)
    for u, unit in enumerate(units):
        if unit[0][1] == 0 and unit[0][0] + 1 < rows:
            project(unit[0][0] + 1)
        following = scores(u + 1) if u + 1 < len(units) else None
        ready = [
            weigh(r, h, (u % 2) * heads + i, best[i]) for i, (r, h) in enumerate(unit)
        ]
        for i, (r, h) in enumerate(unit):
            mix(r, h, (u % 2) * heads + i, *ready[i])
        best = following


def first_kernel(n_chunks, par_ref, *refs):
    chunks = refs[:n_chunks]
    w_ref, q_ref, wt_ref, m_ref, acc_ref, *scratch = refs[n_chunks:]
    rows, cells, width = chunks[0].shape
    scale = 1.0 / math.sqrt(width // HEADS)
    wt_ref[...] = w_ref[...].T
    upper = par_ref[0] == 0
    for r in range(rows):
        for i, x in enumerate([chunks[0][r], jnp.where(upper, chunks[2][r], chunks[1][r])]):
            q = lax.dot_general(
                wt_ref[:width, :], x, (((1,), (1,)), ((), ())), preferred_element_type=jnp.float32
            )
            q = (q * scale).astype(jnp.bfloat16).astype(jnp.float32) * LOG2E
            high = q.astype(jnp.bfloat16)
            q_ref[r, :width, i * cells : (i + 1) * cells] = high
            q_ref[r, width:, i * cells : (i + 1) * cells] = (
                q - high.astype(jnp.float32)
            ).astype(jnp.bfloat16)

    def store(r, h, highest, acc):
        m_ref[r, h : h + 1, :] = highest
        acc_ref[r, h] = acc

    attend_rows(
        chunks, w_ref, wt_ref, q_ref, slice(0, 2 * cells), None, None, store, *scratch
    )


def middle_kernel(n_chunks, *refs):
    chunks = refs[:n_chunks]
    w_ref, wt_ref, q_ref, m_in, acc_in, m_ref, acc_ref, *scratch = refs[n_chunks:]

    def store(r, h, highest, acc):
        m_ref[r, h : h + 1, :] = highest
        acc_ref[r, h] = acc

    attend_rows(
        chunks,
        w_ref,
        wt_ref,
        q_ref,
        slice(0, q_ref.shape[2]),
        lambda r, h: m_in[r, h : h + 1, :],
        lambda r, h: acc_in[r, h],
        store,
        *scratch,
    )


def finish(chunks, w_ref, wt_ref, q_ref, m_in, acc_in, lanes, out_ref, scratch):
    head_width = w_ref.shape[0] // HEADS

    def store(r, h, highest, acc):
        mixed = acc[:head_width] / acc[head_width : head_width + 1]
        out_ref[r, h * head_width : (h + 1) * head_width, :] = mixed.astype(jnp.bfloat16)

    attend_rows(
        chunks,
        w_ref,
        wt_ref,
        q_ref,
        lanes,
        lambda r, h: m_in[r, h : h + 1, lanes],
        lambda r, h: acc_in[r, h, :, lanes],
        store,
        *scratch,
    )


def project(attended_t, w, x):
    y = lax.dot_general(attended_t, w, (((0,), (0,)), ((), ())), preferred_element_type=jnp.float32)
    return (x.astype(jnp.float32) + y).astype(jnp.bfloat16)


def theirs_kernel(n_chunks, *refs):
    *operands, out_ref = refs[n_chunks : n_chunks + 6]
    cells = out_ref.shape[2]
    finish(refs[:n_chunks], *operands, slice(cells, 2 * cells), out_ref, refs[n_chunks + 6 :])


def mine_kernel(n_chunks, par_ref, *refs):
    *operands, x_ref, wo_ref, out_ref = refs[n_chunks : n_chunks + 8]
    *scratch, mixed_ref = refs[n_chunks + 8 :]
    rows, cells, _ = out_ref.shape
    finish(refs[:n_chunks], *operands, slice(0, cells), mixed_ref, scratch)
    for i in range(rows):
        out_ref[i] = project(mixed_ref[i], wo_ref[...], x_ref[par_ref[0] * rows + i])


def attend(kind, chunks, weights, state, parity=None):
    rows, cells, width = chunks[0].shape
    n = len(chunks)
    head_width = width // HEADS
    q_shape = jax.ShapeDtypeStruct((rows, 2 * width, 2 * cells), jnp.bfloat16)
    wt_shape = jax.ShapeDtypeStruct((3 * width, width), jnp.bfloat16)
    m_shape = jax.ShapeDtypeStruct((rows, HEADS, 2 * cells), jnp.float32)
    acc_shape = jax.ShapeDtypeStruct((rows, HEADS, 2 * head_width, 2 * cells), jnp.float32)
    half = jax.ShapeDtypeStruct((rows, width, cells), jnp.bfloat16)
    kernel, outs = {
        "first": (first_kernel, (q_shape, wt_shape, m_shape, acc_shape)),
        "middle": (middle_kernel, (m_shape, acc_shape)),
        "theirs": (theirs_kernel, (half,)),
        "mine": (mine_kernel, (jax.ShapeDtypeStruct((rows, cells, width), jnp.bfloat16),)),
    }[kind]
    scores = rows * HEADS * n * cells * 2 * cells
    operands = [*chunks, *weights, *state]
    heads = max(1, min(HEADS, UNIT // (n * cells)))
    n_queries = 2 * cells if kind in ("first", "middle") else cells
    vmem = pl.BlockSpec(memory_space=pltpu.VMEM)

    scratch = [
        pltpu.VMEM((2 * heads, n * cells, n_queries), jnp.float32),
        pltpu.VMEM((2 * heads, n * cells, n_queries), jnp.bfloat16),
        pltpu.VMEM((2, 2 * width, n * cells), jnp.bfloat16),
        pltpu.VMEM((2, n * cells, 2 * width), jnp.bfloat16),
    ]
    if kind == "mine":
        scratch.append(pltpu.VMEM(half.shape, half.dtype))

    def body(*refs):
        kernel(n, *refs)

    in_specs = [vmem] * len(operands)
    if parity is not None:
        operands.insert(0, parity)
        in_specs.insert(0, pl.BlockSpec(memory_space=pltpu.SMEM))

    return pl.pallas_call(
        body,
        in_specs=in_specs,
        out_specs=(vmem,) * len(outs),
        out_shape=outs,
        scratch_shapes=scratch,
        compiler_params=pltpu.CompilerParams(vmem_limit_bytes=LARGE),
        cost_estimate=pl.CostEstimate(
            flops=scores * 2 * 160 * n_queries // (2 * cells), bytes_accessed=1_000_000, transcendentals=scores
        ),
        name="attend_" + kind,
    )(*operands)


def out_kernel(par_ref, x_ref, done_ref, other_ref, w_ref, o_ref):
    rows = done_ref.shape[0]
    start = par_ref[0] * rows
    for i in range(rows):
        o_ref[start + i] = done_ref[i]
        o_ref[rows - start + i] = project(other_ref[i], w_ref[...], x_ref[rows - start + i])


def project_out(parity, fields, done, other, w_out):
    vmem = pl.BlockSpec(memory_space=pltpu.VMEM)
    return pl.pallas_call(
        out_kernel,
        out_shape=jax.ShapeDtypeStruct(fields.shape, fields.dtype),
        in_specs=[pl.BlockSpec(memory_space=pltpu.SMEM), vmem, vmem, vmem, vmem],
        out_specs=vmem,
        compiler_params=pltpu.CompilerParams(vmem_limit_bytes=SMALL),
        cost_estimate=pl.CostEstimate(flops=12_000_000, bytes_accessed=600_000, transcendentals=0),
        name="project_out",
    )(parity, fields, done, other, w_out)


def body(fields, norm_gain, w_qkv, w_out):
    size = lax.axis_size("lon")
    width = fields.shape[2]
    position = lax.axis_index("lon")
    parity = (position % 2).astype(jnp.int32).reshape(1)

    def shift(block, by):
        return lax.ppermute(block, "lon", [(i, (i + by) % size) for i in range(size)])

    def swap(block):
        return lax.ppermute(block, "lon", [(i, i ^ 1) for i in range(size)])

    own, other = layer_norm_split(parity, fields, norm_gain)
    levels = size // 4
    b = [shift(other, 1), shift(other, -1)]
    a = [shift(own, 2), shift(own, -2)]
    first = [own, *b]
    b = [shift(b[0], 2), shift(b[1], -2)]
    q, wt, *state = attend("first", first, (w_qkv,), (), parity)
    for level in range(1, levels):
        a, state = lax.optimization_barrier((a, state))
        chunks = a
        a = [shift(a[0], 2), shift(a[1], -2)] if level < levels - 1 else [shift(a[1], -2)]
        state = attend("middle", chunks, (w_qkv, wt), (q, *state))
        b, state = lax.optimization_barrier((b, state))
        chunks = b
        b = [shift(b[0], 2), shift(b[1], -2)] if level < levels - 1 else []
        state = attend("middle", chunks, (w_qkv, wt), (q, *state))
    (theirs,) = attend("theirs", a, (w_qkv, wt), (q, *state))
    back = swap(theirs)
    (mine,) = attend("mine", a, (w_qkv, wt), (q, *state, fields, w_out), parity)
    return project_out(parity, fields, mine, back, w_out)


def solution(mesh):
    return jax.shard_map(
        body,
        mesh=mesh,
        in_specs=(P(("groups", "lat"), "lon", None), P(), P(), P()),
        out_specs=P(("groups", "lat"), "lon", None),
        check_vma=False,
    )
```
